32 devices in a mesh: rep: 2 (over x), mp: 4 (over z), tok: 4 (over y, core).
Axes of the slice: x: 2, y: 2, z: 4, core: 2. Of those that a mesh axis runs over, the one named last changes fastest.
Arguments:
- hidden_in: bfloat16 [8192, 1536], P(('rep', 'tok', 'mp')), parts along dimension 0
- seg_ids: int32 [8192], P(('rep', 'tok', 'mp')), parts along dimension 0
- expert_ids: int32 [8192, 2], P(('rep', 'tok', 'mp')), parts along dimension 0
- expert_gates: float32 [8192, 2], P(('rep', 'tok', 'mp')), parts along dimension 0
- w_query: bfloat16 [2, 1536, 24, 64], P(None, 'tok', 'mp')
- w_key: bfloat16 [2, 1536, 8, 64], P(None, 'tok', 'mp')
- w_value: bfloat16 [2, 1536, 8, 64], P(None, 'tok', 'mp')
- w_out: bfloat16 [2, 24, 64, 1536], P(None, 'mp', None, 'tok')
- w_gate: bfloat16 [2, 40, 1536, 512], P(None, None, 'tok', 'mp')
- w_up: bfloat16 [2, 40, 1536, 512], P(None, None, 'tok', 'mp')
- w_down: bfloat16 [2, 40, 512, 1536], P(None, None, 'mp', 'tok')
- gain_attn: bfloat16 [2, 1536], replicated
- gain_mlp: bfloat16 [2, 1536], replicated
Outputs:
- output: float32 [8192, 1536], P(('rep', 'tok', 'mp')), parts along dimension 0
There are 2 independent parts. The reference program is written for one: setup_inputs(seed, part) draws one part's arguments, and reference() takes and returns one part's arrays. A program takes and returns all parts, laid end to end along the dimension named above; an argument that names none is the same for every part.
All inputs are finite; a program needn't handle non-finite values.
Results may differ from the reference program's by a relative error of at most 0.0149105.
Values are sent between devices in bfloat16 or wider.
A program may use at most 1 GiB of HBM per device.

```python
import jax
import jax.numpy as jnp
from jax import lax

TOKENS = 4096
SHARDS = 4
HIDDEN = 1536
FFN_WIDTH = 512
Q_HEADS = 24
KV_HEADS = 8
HEAD_DIM = 64
EXPERTS = 40
NUM_LAYERS = 2
REQ_CUTS = 3

SHARD_LEN = TOKENS // SHARDS
QUERY_BLOCK = min(SHARD_LEN, 256)
EPS = 1e-5
ROPE_BASE = 10000.0


def normal_weight(key, shape, scale):
    return (jax.random.normal(key, shape, jnp.float32) * scale).astype(jnp.bfloat16)


def setup_inputs(seed: int = 0, part: int = 0) -> dict:
    base_key = jax.random.key(seed)
    part_keys = jax.random.split(jax.random.fold_in(base_key, part), 5)
    weight_keys = jax.random.split(jax.random.key(seed + 1), 9)
    hidden_in = jax.random.normal(part_keys[0], (TOKENS, HIDDEN), jnp.float32).astype(jnp.bfloat16)
    cut_points = jax.random.randint(part_keys[1], (SHARDS, 1, REQ_CUTS), 1, SHARD_LEN)
    token_pos = jnp.arange(SHARD_LEN, dtype=jnp.int32)[None, :, None]
    req_index = jnp.sum((token_pos >= cut_points).astype(jnp.int32), axis=-1)
    shard_base = jnp.arange(SHARDS, dtype=jnp.int32)[:, None] * (REQ_CUTS + 1)
    seg_ids = (shard_base + req_index).reshape(TOKENS).astype(jnp.int32)
    first_pick = jax.random.permutation(part_keys[2], jnp.arange(TOKENS, dtype=jnp.int32) % EXPERTS)
    pick_shift = jax.random.randint(part_keys[3], (TOKENS,), 1, EXPERTS)
    second_pick = (first_pick + pick_shift) % EXPERTS
    expert_ids = jnp.stack([first_pick, second_pick], axis=1).astype(jnp.int32)
    top_share = jax.random.uniform(part_keys[4], (TOKENS,), jnp.float32, 0.3, 0.9)
    expert_gates = jnp.stack([top_share, 1.0 - top_share], axis=1)
    qk_scale = 1.4 * HIDDEN ** -0.5
    return {
        'hidden_in': hidden_in,
        'seg_ids': seg_ids,
        'expert_ids': expert_ids,
        'expert_gates': expert_gates,
        'w_query': normal_weight(weight_keys[0], (NUM_LAYERS, HIDDEN, Q_HEADS, HEAD_DIM), qk_scale),
        'w_key': normal_weight(weight_keys[1], (NUM_LAYERS, HIDDEN, KV_HEADS, HEAD_DIM), qk_scale),
        'w_value': normal_weight(weight_keys[2], (NUM_LAYERS, HIDDEN, KV_HEADS, HEAD_DIM), HIDDEN ** -0.5),
        'w_out': normal_weight(weight_keys[3], (NUM_LAYERS, Q_HEADS, HEAD_DIM, HIDDEN), 2.0 * (Q_HEADS * HEAD_DIM) ** -0.5),
        'w_gate': normal_weight(weight_keys[4], (NUM_LAYERS, EXPERTS, HIDDEN, FFN_WIDTH), HIDDEN ** -0.5),
        'w_up': normal_weight(weight_keys[5], (NUM_LAYERS, EXPERTS, HIDDEN, FFN_WIDTH), HIDDEN ** -0.5),
        'w_down': normal_weight(weight_keys[6], (NUM_LAYERS, EXPERTS, FFN_WIDTH, HIDDEN), FFN_WIDTH ** -0.5),
        'gain_attn': jax.random.uniform(weight_keys[7], (NUM_LAYERS, HIDDEN), jnp.float32, 0.5, 1.5).astype(jnp.bfloat16),
        'gain_mlp': jax.random.uniform(weight_keys[8], (NUM_LAYERS, HIDDEN), jnp.float32, 0.5, 1.5).astype(jnp.bfloat16),
    }


def rms_norm(residual, gain):
    inv_rms = lax.rsqrt(jnp.mean(residual * residual, axis=-1, keepdims=True) + EPS)
    return (residual * inv_rms * gain.astype(jnp.float32)).astype(jnp.bfloat16)


def request_positions(seg_shard):
    token_index = jnp.arange(SHARD_LEN, dtype=jnp.int32)
    is_start = jnp.concatenate([jnp.ones((1,), dtype=jnp.bool_), seg_shard[1:] != seg_shard[:-1]])
    start_index = lax.cummax(jnp.where(is_start, token_index, 0), axis=0)
    return token_index - start_index


def apply_rope(vectors, positions):
    half_dim = HEAD_DIM // 2
    inv_freq = jnp.power(ROPE_BASE, -jnp.arange(half_dim, dtype=jnp.float32) * 2.0 / HEAD_DIM)
    angles = positions.astype(jnp.float32)[:, None, None] * inv_freq
    cosines = jnp.cos(angles)
    sines = jnp.sin(angles)
    first_half = vectors[..., :half_dim]
    second_half = vectors[..., half_dim:]
    return jnp.concatenate([first_half * cosines - second_half * sines, second_half * cosines + first_half * sines], axis=-1)


def shard_attention(h_shard, seg_shard, q_weight, k_weight, v_weight):
    groups = Q_HEADS // KV_HEADS
    positions = request_positions(seg_shard)
    q_proj = jnp.dot(h_shard, q_weight.reshape(HIDDEN, Q_HEADS * HEAD_DIM), preferred_element_type=jnp.float32)
    k_proj = jnp.dot(h_shard, k_weight.reshape(HIDDEN, KV_HEADS * HEAD_DIM), preferred_element_type=jnp.float32)
    v_proj = jnp.dot(h_shard, v_weight.reshape(HIDDEN, KV_HEADS * HEAD_DIM), preferred_element_type=jnp.float32)
    q_rot = apply_rope(q_proj.reshape(SHARD_LEN, Q_HEADS, HEAD_DIM), positions).astype(jnp.bfloat16)
    k_rot = apply_rope(k_proj.reshape(SHARD_LEN, KV_HEADS, HEAD_DIM), positions).astype(jnp.bfloat16)
    keys32 = k_rot.astype(jnp.float32)
    values32 = v_proj.astype(jnp.bfloat16).astype(jnp.float32).reshape(SHARD_LEN, KV_HEADS, HEAD_DIM)
    token_index = jnp.arange(SHARD_LEN, dtype=jnp.int32)
    num_blocks = SHARD_LEN // QUERY_BLOCK
    q_blocks = q_rot.reshape(num_blocks, QUERY_BLOCK, KV_HEADS, groups, HEAD_DIM)

    def one_block(block_in):
        q_block, seg_block, index_block = block_in
        scores = jnp.einsum('bhgd,shd->hgbs', q_block.astype(jnp.float32), keys32) * HEAD_DIM ** -0.5
        allowed = (seg_block[:, None] == seg_shard[None, :]) & (token_index[None, :] <= index_block[:, None])
        attn_prob = jax.nn.softmax(jnp.where(allowed, scores, -1e30), axis=-1)
        attn_prob = attn_prob.astype(jnp.bfloat16).astype(jnp.float32)
        attn_out = jnp.einsum('hgbs,shd->bhgd', attn_prob, values32)
        return attn_out.astype(jnp.bfloat16).reshape(QUERY_BLOCK, Q_HEADS * HEAD_DIM)

    block_outs = lax.map(one_block, (q_blocks, seg_shard.reshape(num_blocks, QUERY_BLOCK), token_index.reshape(num_blocks, QUERY_BLOCK)))
    return block_outs.reshape(SHARD_LEN, Q_HEADS * HEAD_DIM)


def expert_mix(normed, expert_ids, expert_gates, gate_weight, up_weight, down_weight):
    def one_expert(mix_sum, expert_in):
        gate_mat, up_mat, down_mat, expert_num = expert_in
        gate_pre = jnp.dot(normed, gate_mat, preferred_element_type=jnp.float32)
        up_pre = jnp.dot(normed, up_mat, preferred_element_type=jnp.float32)
        hidden_act = (jax.nn.silu(gate_pre) * up_pre).astype(jnp.bfloat16)
        down_out = jnp.dot(hidden_act, down_mat, preferred_element_type=jnp.float32)
        route_weight = jnp.sum(jnp.where(expert_ids == expert_num, expert_gates, 0.0), axis=1)
        return mix_sum + route_weight[:, None] * down_out, None

    start_sum = jnp.zeros((normed.shape[0], HIDDEN), jnp.float32)
    mix_sum, _ = lax.scan(one_expert, start_sum, (gate_weight, up_weight, down_weight, jnp.arange(EXPERTS, dtype=jnp.int32)))
    return mix_sum


def reference(hidden_in, seg_ids, expert_ids, expert_gates, w_query, w_key, w_value, w_out, w_gate, w_up, w_down, gain_attn, gain_mlp):
    seg_shards = seg_ids.reshape(SHARDS, SHARD_LEN)

    def one_layer(residual, layer_in):
        q_weight, k_weight, v_weight, o_weight, gate_weight, up_weight, down_weight, attn_gain, mlp_gain = layer_in
        normed = rms_norm(residual, attn_gain).reshape(SHARDS, SHARD_LEN, HIDDEN)
        attn_out = lax.map(lambda shard_in: shard_attention(shard_in[0], shard_in[1], q_weight, k_weight, v_weight), (normed, seg_shards))
        attn_out = attn_out.reshape(TOKENS, Q_HEADS * HEAD_DIM)
        residual = residual + jnp.dot(attn_out, o_weight.reshape(Q_HEADS * HEAD_DIM, HIDDEN), preferred_element_type=jnp.float32)
        normed = rms_norm(residual, mlp_gain)
        residual = residual + expert_mix(normed, expert_ids, expert_gates, gate_weight, up_weight, down_weight)
        return residual, None

    final, _ = lax.scan(one_layer, hidden_in.astype(jnp.float32), (w_query, w_key, w_value, w_out, w_gate, w_up, w_down, gain_attn, gain_mlp))
    return final
```

```python
import jax
import jax.numpy as jnp
from jax import lax
from jax.experimental import pallas as pl
from jax.experimental.pallas import tpu as pltpu
from jax.sharding import PartitionSpec as P


EPS = 1e-5
ROPE_BASE = 10000.0
ROW_ALIGN = 16
ROW_BLOCK = 64
GATHER_ROWS = 256


def rms_norm(residual, gain):
    inv_rms = lax.rsqrt(jnp.mean(residual * residual, axis=-1, keepdims=True) + EPS)
    return (residual * inv_rms * gain.astype(jnp.float32)).astype(jnp.bfloat16)


def request_positions(seg_rows):
    token_index = jnp.arange(seg_rows.shape[-1], dtype=jnp.int32)
    is_start = jnp.concatenate([jnp.ones(seg_rows.shape[:-1] + (1,), dtype=jnp.bool_), seg_rows[..., 1:] != seg_rows[..., :-1]], axis=-1)
    start_index = lax.cummax(jnp.where(is_start, token_index, 0), axis=seg_rows.ndim - 1)
    return token_index - start_index


def rope_tables(positions, head_dim):
    inv_freq = jnp.power(ROPE_BASE, -jnp.arange(head_dim // 2, dtype=jnp.float32) * 2.0 / head_dim)
    angles = positions.astype(jnp.float32)[..., None] * inv_freq
    return jnp.cos(angles)[..., None, :], jnp.sin(angles)[..., None, :]


def apply_rope(vectors, cosines, sines):
    half_dim = vectors.shape[-1] // 2
    first_half = vectors[..., :half_dim]
    second_half = vectors[..., half_dim:]
    return jnp.concatenate([first_half * cosines - second_half * sines, second_half * cosines + first_half * sines], axis=-1)


def block_attention(q_rot, k_rot, v_all, seg_query, query_index, seg_keys, key_index):
    n_query, kv_heads, groups, head_dim = q_rot.shape
    block = min(n_query, 512)
    num_blocks = n_query // block
    scale = head_dim ** -0.5

    def one_block(block_in):
        q_block, seg_block, index_block = block_in
        scores = jnp.einsum('bhgd,shd->hgbs', q_block, k_rot, preferred_element_type=jnp.float32) * scale
        allowed = (seg_block[:, None] == seg_keys[None, :]) & (key_index[None, :] <= index_block[:, None])
        attn_prob = jax.nn.softmax(jnp.where(allowed, scores, -1e30), axis=-1).astype(jnp.bfloat16)
        return jnp.einsum('hgbs,shd->bhgd', attn_prob, v_all, preferred_element_type=jnp.float32).astype(jnp.bfloat16)

    block_outs = lax.map(one_block, (q_rot.reshape(num_blocks, block, kv_heads, groups, head_dim), seg_query.reshape(num_blocks, block), query_index.reshape(num_blocks, block)))
    return block_outs.reshape(n_query, kv_heads * groups, head_dim)


def moe_kernel(place_ref, start_ref, count_ref, pos_ref, gate_ref, pos0_ref, pos1_ref, h_ref, *rest):
    weights, (out_ref, x_ref, d_ref) = rest[:24], rest[24:]
    step = pl.program_id(0)
    my_slice = place_ref[1]
    parts, slices, part_rows, width = h_ref.shape
    rows = x_ref.shape[1]

    @pl.when(step == 0)
    def _():
        def gather_rows(chunk, carry):
            base = pl.multiple_of(chunk * GATHER_ROWS, GATHER_ROWS)
            row_ids = base + lax.broadcasted_iota(jnp.int32, (GATHER_ROWS, part_rows), 0)
            picks = [((pos0_ref[part] == row_ids) | (pos1_ref[part] == row_ids)).astype(jnp.float32).astype(jnp.bfloat16) for part in range(parts)]
            for k in range(slices):
                acc = jnp.zeros((GATHER_ROWS, width), jnp.float32)
                for part in range(parts):
                    acc += jnp.dot(picks[part], h_ref[part, my_slice ^ k], preferred_element_type=jnp.float32)
                x_ref[k, pl.ds(base, GATHER_ROWS), :] = acc.astype(jnp.bfloat16)
            return carry

        lax.fori_loop(0, rows // GATHER_ROWS, gather_rows, 0)

    def one_expert(rank, gate_w, up_w, down_w):
        start = start_ref[rank]

        def one_block(block, carry):
            base = pl.multiple_of(start + block * ROW_BLOCK, ROW_ALIGN)
            gate_pre = jnp.zeros((ROW_BLOCK, gate_w[0].shape[1]), jnp.float32)
            up_pre = jnp.zeros((ROW_BLOCK, gate_w[0].shape[1]), jnp.float32)
            for k in range(slices):
                x_rows = x_ref[k, pl.ds(base, ROW_BLOCK), :]
                gate_pre += jnp.dot(x_rows, gate_w[k][...], preferred_element_type=jnp.float32)
                up_pre += jnp.dot(x_rows, up_w[k][...], preferred_element_type=jnp.float32)
            act = (jax.nn.silu(gate_pre) * up_pre).astype(jnp.bfloat16)
            for k in range(slices):
                d_ref[k, pl.ds(base, ROW_BLOCK), :] = jnp.dot(act, down_w[k][...], preferred_element_type=jnp.float32)
            return carry

        lax.fori_loop(0, count_ref[rank], one_block, 0)

    own_half, other_half = [0, 2, 4, 6], [1, 3, 5, 7]
    for half, order in enumerate((own_half, other_half)):
        one_expert(2 * step + half, [weights[j] for j in order], [weights[8 + j] for j in order], [weights[16 + j] for j in order])

    @pl.when(step == pl.num_programs(0) - 1)
    def _():
        for part in range(parts):
            def mix_rows(group, carry):
                base = pl.multiple_of(group * 8, 8)
                for u in range(8):
                    pair = 2 * (part * part_rows + base + u)
                    p0, p1 = pos_ref[pair], pos_ref[pair + 1]
                    g0, g1 = gate_ref[pair], gate_ref[pair + 1]
                    for k in range(slices):
                        out_ref[part * slices + (my_slice ^ k), pl.ds(base + u, 1), :] = d_ref[k, pl.ds(p0, 1), :] * g0 + d_ref[k, pl.ds(p1, 1), :] * g1
                return carry

            lax.fori_loop(0, part_rows // 8, mix_rows, 0)


def expert_mix(layer, place, route, h_all, weight_sets):
    starts, blocks, pair_pos, pair_gate, pos0, pos1, rows = route
    parts, slices, part_rows, width = h_all.shape
    half = weight_sets[0][2].shape[0]

    def whole(ndim):
        return lambda i, *_: (0,) * ndim

    in_specs = [pl.BlockSpec(memory_space=pltpu.SMEM), pl.BlockSpec(pos0.shape, whole(3)), pl.BlockSpec(pos1.shape, whole(3)), pl.BlockSpec(h_all.shape, whole(4))]
    operands = [pair_gate, pos0, pos1, h_all]
    for own, peer, y_half, x_half, y_far, x_far in weight_sets:
        block = own.shape[2:]
        near = pl.BlockSpec((None, None) + block, lambda i, place, *_: (layer, half * place[0] + i, 0, 0))
        far = pl.BlockSpec((None, None) + block, lambda i, place, *_: (layer, half * (1 - place[0]) + i, 0, 0))
        piece = pl.BlockSpec((None,) + block, lambda i, *_: (i, 0, 0))
        in_specs += [near, far, near, far, piece, piece, piece, piece]
        operands += [own, own, peer, peer, y_half, x_half, y_far, x_far]
    flops = 2 * rows * parts * part_rows * slices * width + 6 * 2 * parts * part_rows * slices * width * 128
    return pl.pallas_call(
        moe_kernel,
        grid_spec=pltpu.PrefetchScalarGridSpec(
            num_scalar_prefetch=4,
            grid=(half,),
            in_specs=in_specs,
            out_specs=pl.BlockSpec((parts * slices, part_rows, width), whole(3)),
            scratch_shapes=[pltpu.VMEM((slices, rows, width), jnp.bfloat16), pltpu.VMEM((slices, rows, width), jnp.float32)],
        ),
        out_shape=jax.ShapeDtypeStruct((parts * slices, part_rows, width), jnp.float32),
        compiler_params=pltpu.CompilerParams(vmem_limit_bytes=60 * 1024 * 1024, dimension_semantics=("arbitrary",)),
        cost_estimate=pl.CostEstimate(flops=flops * 4, bytes_accessed=60_000_000, transcendentals=0),
        name="expert_mix",
    )(place, starts, blocks, pair_pos, *operands)


def routing(ids, gates, num_experts, my_rep, parts, part_rows):
    half = num_experts // 2
    pairs = ids.shape[0]
    rank = 2 * (ids % half) + (ids // half != my_rep).astype(jnp.int32)
    hits = (rank[:, None] == jnp.arange(num_experts, dtype=jnp.int32)[None, :])
    index = jnp.arange(pairs, dtype=jnp.int32)
    before = (index[:, None] > index[None, :]).astype(jnp.bfloat16)
    place_in = jnp.dot(before, hits.astype(jnp.bfloat16), preferred_element_type=jnp.float32)
    counts = jnp.sum(hits.astype(jnp.int32), axis=0)
    padded = (counts + (ROW_ALIGN - 1)) // ROW_ALIGN * ROW_ALIGN
    order = jnp.arange(num_experts, dtype=jnp.int32)
    starts = jnp.sum(jnp.where(order[None, :] < order[:, None], padded[None, :], 0), axis=1)
    blocks = (counts + (ROW_BLOCK - 1)) // ROW_BLOCK
    pair_pos = jnp.sum(jnp.where(hits, place_in.astype(jnp.int32) + starts[None, :], 0), axis=1)
    two = pair_pos.reshape(parts, part_rows, 2)
    rows = pairs + num_experts * (ROW_ALIGN - 1) + ROW_BLOCK
    rows = (rows + GATHER_ROWS - 1) // GATHER_ROWS * GATHER_ROWS
    return starts, blocks, pair_pos, gates.reshape(pairs), two[:, None, :, 0], two[:, None, :, 1], rows


def solution(mesh):
    n_tok, n_mp = mesh.shape['tok'], mesh.shape['mp']
    token_spec = P(('rep', 'tok', 'mp'))
    row_spec = P(('rep', 'tok', 'mp'), None)
    head_weight = P(None, 'tok', 'mp', None)
    in_specs = (row_spec, token_spec, row_spec, row_spec, head_weight, head_weight, head_weight, P(None, 'mp', None, 'tok'), P(None, None, 'tok', 'mp'), P(None, None, 'tok', 'mp'), P(None, None, 'mp', 'tok'), P(None, None), P(None, None))
    swap_perm = [(m * n_tok + t, t * n_tok + m) for t in range(n_tok) for m in range(n_mp)]
    core_perm = [(t, t ^ 1) for t in range(n_tok)]
    y_perm = [(t, t ^ 2) for t in range(n_tok)]
    x_perm = [(0, 1), (1, 0)]

    def swap_roles(value):
        return lax.ppermute(value, ('mp', 'tok'), swap_perm)

    def device_step(hidden_in, seg_ids, expert_ids, expert_gates, w_query, w_key, w_value, w_out, w_gate, w_up, w_down, gain_attn, gain_mlp):
        num_layers, slice_width, q_local, head_dim = w_query.shape
        kv_local = w_key.shape[2]
        groups = q_local // kv_local
        num_experts = w_gate.shape[1]
        half = num_experts // 2
        part_rows = hidden_in.shape[0]
        my_rep, my_tok, my_mp = lax.axis_index('rep'), lax.axis_index('tok'), lax.axis_index('mp')
        place = jnp.stack([my_rep, my_tok]).astype(jnp.int32)
        hidden_width = slice_width * n_tok
        attn_cols = (q_local + 2 * kv_local) * head_dim

        swapped = swap_roles(hidden_in)
        residual = swapped.astype(jnp.float32)
        attn_packs = []
        for layer in range(num_layers):
            qkv = jnp.concatenate([w_query[layer], w_key[layer], w_value[layer]], axis=1).reshape(slice_width, attn_cols)
            pack = jnp.concatenate([qkv, w_out[layer].reshape(q_local * head_dim, slice_width)], axis=1)
            attn_packs.append(swap_roles(pack))

        expert_weights = (w_gate, w_up, w_down)
        peers = []
        for own in expert_weights:
            peers.append(lax.ppermute(own, 'tok', core_perm))
        layer_sets = []
        for layer in range(num_layers):
            sets = []
            for own, peer in zip(expert_weights, peers):
                mine = lax.dynamic_slice(own, (layer, my_rep * half, 0, 0), (1, half) + own.shape[2:])[0]
                y_half = lax.ppermute(mine, 'tok', y_perm)
                x_half = lax.ppermute(y_half, 'rep', x_perm)
                y_far = lax.ppermute(y_half, 'tok', core_perm)
                x_far = lax.ppermute(x_half, 'tok', core_perm)
                sets.append((own, peer, y_half, x_half, y_far, x_far))
            layer_sets.append(sets)

        seg_all = lax.all_gather(seg_ids, ('tok', 'mp'), axis=0)
        pair_info = jnp.concatenate([expert_ids.astype(jnp.float32), expert_gates], axis=1)
        pair_all = lax.all_gather(pair_info, ('tok', 'mp'), axis=0).reshape(n_tok, n_mp, part_rows, 4)
        seg_full = lax.dynamic_index_in_dim(seg_all.reshape(n_tok, n_mp * part_rows), my_mp, axis=0, keepdims=False)
        pair_mine = lax.dynamic_index_in_dim(pair_all, my_tok, axis=1, keepdims=False).reshape(n_tok * part_rows, 4)
        route = routing(pair_mine[:, :2].astype(jnp.int32).reshape(-1), pair_mine[:, 2:], num_experts, my_rep, n_tok, part_rows)
        seq_len = seg_full.shape[0]
        token_index = jnp.arange(seq_len, dtype=jnp.int32)
        cosines, sines = rope_tables(request_positions(seg_full), head_dim)
        for layer in range(num_layers):
            pack = lax.all_gather(attn_packs[layer], 'mp', axis=0)
            qkv_weight = pack[:, :, :attn_cols].reshape(hidden_width, attn_cols)
            o_weight = pack[:, :, attn_cols:]
            normed = rms_norm(residual, gain_attn[layer])
            normed = lax.all_gather(normed, 'tok', axis=0, tiled=True)
            qkv = jnp.dot(normed, qkv_weight, preferred_element_type=jnp.float32)
            qkv = qkv.reshape(seq_len, q_local + 2 * kv_local, head_dim)
            rotated = apply_rope(qkv[:, :q_local + kv_local], cosines, sines).astype(jnp.bfloat16)
            q_rot = rotated[:, :q_local].reshape(seq_len, kv_local, groups, head_dim)
            k_rot = rotated[:, q_local:]
            v_all = qkv[:, q_local + kv_local:].astype(jnp.bfloat16)
            attn_out = block_attention(q_rot, k_rot, v_all, seg_full, token_index, seg_full, token_index)
            attn_part = jnp.einsum('sk,tkw->stw', attn_out.reshape(seq_len, q_local * head_dim), o_weight, preferred_element_type=jnp.float32)
            attn_part = attn_part.reshape(seq_len, hidden_width)
            residual = residual + lax.psum_scatter(attn_part, 'tok', scatter_dimension=0, tiled=True)
            normed = rms_norm(residual, gain_mlp[layer])
            normed = normed.reshape(part_rows, n_tok, slice_width).transpose(1, 0, 2)
            h_all = lax.all_gather(normed, 'mp', axis=0)
            mix_part = expert_mix(layer, place, route, h_all, layer_sets[layer])
            mix = lax.psum_scatter(mix_part, 'mp', scatter_dimension=0, tiled=True)
            residual = residual + mix.transpose(1, 0, 2).reshape(part_rows, hidden_width)
        return swap_roles(residual)

    return jax.shard_map(device_step, mesh=mesh, in_specs=in_specs, out_specs=row_spec, check_vma=False)
```

```python
import jax
import jax.numpy as jnp
from jax import lax
from jax.experimental import pallas as pl
from jax.experimental.pallas import tpu as pltpu
from jax.sharding import PartitionSpec as P


EPS = 1e-5
ROPE_BASE = 10000.0
ROW_ALIGN = 16
ROW_BLOCK = 64
GATHER_ROWS = 256


def rms_norm(residual, gain):
    inv_rms = lax.rsqrt(jnp.mean(residual * residual, axis=-1, keepdims=True) + EPS)
    return (residual * inv_rms * gain.astype(jnp.float32)).astype(jnp.bfloat16)


def request_positions(seg_rows):
    token_index = jnp.arange(seg_rows.shape[-1], dtype=jnp.int32)
    is_start = jnp.concatenate([jnp.ones(seg_rows.shape[:-1] + (1,), dtype=jnp.bool_), seg_rows[..., 1:] != seg_rows[..., :-1]], axis=-1)
    start_index = lax.cummax(jnp.where(is_start, token_index, 0), axis=seg_rows.ndim - 1)
    return token_index - start_index


def rope_tables(positions, head_dim):
    inv_freq = jnp.power(ROPE_BASE, -jnp.arange(head_dim // 2, dtype=jnp.float32) * 2.0 / head_dim)
    angles = positions.astype(jnp.float32)[..., None] * inv_freq
    return jnp.cos(angles)[..., None, :], jnp.sin(angles)[..., None, :]


def apply_rope(vectors, cosines, sines):
    half_dim = vectors.shape[-1] // 2
    first_half = vectors[..., :half_dim]
    second_half = vectors[..., half_dim:]
    return jnp.concatenate([first_half * cosines - second_half * sines, second_half * cosines + first_half * sines], axis=-1)


def block_attention(q_rot, k_rot, v_all, seg_query, query_index, seg_keys, key_index):
    n_query, kv_heads, groups, head_dim = q_rot.shape
    block = min(n_query, 512)
    num_blocks = n_query // block
    scale = head_dim ** -0.5

    def one_block(block_in):
        q_block, seg_block, index_block = block_in
        scores = jnp.einsum('bhgd,shd->hgbs', q_block, k_rot, preferred_element_type=jnp.float32) * scale
        allowed = (seg_block[:, None] == seg_keys[None, :]) & (key_index[None, :] <= index_block[:, None])
        attn_prob = jax.nn.softmax(jnp.where(allowed, scores, -1e30), axis=-1).astype(jnp.bfloat16)
        return jnp.einsum('hgbs,shd->bhgd', attn_prob, v_all, preferred_element_type=jnp.float32).astype(jnp.bfloat16)

    block_outs = lax.map(one_block, (q_rot.reshape(num_blocks, block, kv_heads, groups, head_dim), seg_query.reshape(num_blocks, block), query_index.reshape(num_blocks, block)))
    return block_outs.reshape(n_query, kv_heads * groups, head_dim)


def moe_kernel(place_ref, start_ref, count_ref, pos_ref, gate_ref, pos0_ref, pos1_ref, h_ref, *rest):
    weights, (out_ref, x_ref, d_ref) = rest[:24], rest[24:]
    step = pl.program_id(0)
    my_slice = place_ref[1]
    parts, slices, part_rows, width = h_ref.shape
    rows = x_ref.shape[1]

    @pl.when(step == 0)
    def _():
        def gather_rows(chunk, carry):
            base = pl.multiple_of(chunk * GATHER_ROWS, GATHER_ROWS)
            row_ids = base + lax.broadcasted_iota(jnp.int32, (GATHER_ROWS, part_rows), 0)
            picks = [((pos0_ref[part] == row_ids) | (pos1_ref[part] == row_ids)).astype(jnp.float32).astype(jnp.bfloat16) for part in range(parts)]
            for k in range(slices):
                acc = jnp.zeros((GATHER_ROWS, width), jnp.float32)
                for part in range(parts):
                    acc += jnp.dot(picks[part], h_ref[part, my_slice ^ k], preferred_element_type=jnp.float32)
                x_ref[k, pl.ds(base, GATHER_ROWS), :] = acc.astype(jnp.bfloat16)
            return carry

        lax.fori_loop(0, rows // GATHER_ROWS, gather_rows, 0)

    def one_expert(rank, gate_w, up_w, down_w):
        start = start_ref[rank]

        def one_block(block, carry):
            base = pl.multiple_of(start + block * ROW_BLOCK, ROW_ALIGN)
            gate_pre = jnp.zeros((ROW_BLOCK, gate_w[0].shape[1]), jnp.float32)
            up_pre = jnp.zeros((ROW_BLOCK, gate_w[0].shape[1]), jnp.float32)
            for k in range(slices):
                x_rows = x_ref[k, pl.ds(base, ROW_BLOCK), :]
                gate_pre += jnp.dot(x_rows, gate_w[k][...], preferred_element_type=jnp.float32)
                up_pre += jnp.dot(x_rows, up_w[k][...], preferred_element_type=jnp.float32)
            act = (jax.nn.silu(gate_pre) * up_pre).astype(jnp.bfloat16)
            for k in range(slices):
                d_ref[k, pl.ds(base, ROW_BLOCK), :] = jnp.dot(act, down_w[k][...], preferred_element_type=jnp.float32)
            return carry

        lax.fori_loop(0, count_ref[rank], one_block, 0)

    own_half, other_half = [0, 2, 4, 6], [1, 3, 5, 7]
    for half, order in enumerate((own_half, other_half)):
        one_expert(2 * step + half, [weights[j] for j in order], [weights[8 + j] for j in order], [weights[16 + j] for j in order])

    @pl.when(step == pl.num_programs(0) - 1)
    def _():
        for part in range(parts):
            def mix_rows(group, carry):
                base = pl.multiple_of(group * 8, 8)
                for u in range(8):
                    pair = 2 * (part * part_rows + base + u)
                    p0, p1 = pos_ref[pair], pos_ref[pair + 1]
                    g0, g1 = gate_ref[pair], gate_ref[pair + 1]
                    for k in range(slices):
                        out_ref[part * slices + (my_slice ^ k), pl.ds(base + u, 1), :] = d_ref[k, pl.ds(p0, 1), :] * g0 + d_ref[k, pl.ds(p1, 1), :] * g1
                return carry

            lax.fori_loop(0, part_rows // 8, mix_rows, 0)


def expert_mix(layer, place, route, h_all, weight_sets):
    starts, blocks, pair_pos, pair_gate, pos0, pos1, rows = route
    parts, slices, part_rows, width = h_all.shape
    half = weight_sets[0][2].shape[0]

    def whole(ndim):
        return lambda i, *_: (0,) * ndim

    in_specs = [pl.BlockSpec(memory_space=pltpu.SMEM), pl.BlockSpec(pos0.shape, whole(3)), pl.BlockSpec(pos1.shape, whole(3)), pl.BlockSpec(h_all.shape, whole(4))]
    operands = [pair_gate, pos0, pos1, h_all]
    for own, peer, y_half, x_half, y_far, x_far in weight_sets:
        block = own.shape[2:]
        near = pl.BlockSpec((None, None) + block, lambda i, place, *_: (layer, half * place[0] + i, 0, 0))
        far = pl.BlockSpec((None, None) + block, lambda i, place, *_: (layer, half * (1 - place[0]) + i, 0, 0))
        piece = pl.BlockSpec((None,) + block, lambda i, *_: (i, 0, 0))
        in_specs += [near, far, near, far, piece, piece, piece, piece]
        operands += [own, own, peer, peer, y_half, x_half, y_far, x_far]
    flops = 2 * rows * parts * part_rows * slices * width + 6 * 2 * parts * part_rows * slices * width * 128
    return pl.pallas_call(
        moe_kernel,
        grid_spec=pltpu.PrefetchScalarGridSpec(
            num_scalar_prefetch=4,
            grid=(half,),
            in_specs=in_specs,
            out_specs=pl.BlockSpec((parts * slices, part_rows, width), whole(3)),
            scratch_shapes=[pltpu.VMEM((slices, rows, width), jnp.bfloat16), pltpu.VMEM((slices, rows, width), jnp.float32)],
        ),
        out_shape=jax.ShapeDtypeStruct((parts * slices, part_rows, width), jnp.float32),
        compiler_params=pltpu.CompilerParams(vmem_limit_bytes=60 * 1024 * 1024, dimension_semantics=("arbitrary",)),
        cost_estimate=pl.CostEstimate(flops=flops * 4, bytes_accessed=60_000_000, transcendentals=0),
        name="expert_mix",
    )(place, starts, blocks, pair_pos, *operands)


def routing(ids, gates, num_experts, my_rep, parts, part_rows):
    half = num_experts // 2
    pairs = ids.shape[0]
    rank = 2 * (ids % half) + (ids // half != my_rep).astype(jnp.int32)
    hits = (rank[:, None] == jnp.arange(num_experts, dtype=jnp.int32)[None, :])
    index = jnp.arange(pairs, dtype=jnp.int32)
    before = (index[:, None] > index[None, :]).astype(jnp.bfloat16)
    place_in = jnp.dot(before, hits.astype(jnp.bfloat16), preferred_element_type=jnp.float32)
    counts = jnp.sum(hits.astype(jnp.int32), axis=0)
    padded = (counts + (ROW_ALIGN - 1)) // ROW_ALIGN * ROW_ALIGN
    order = jnp.arange(num_experts, dtype=jnp.int32)
    starts = jnp.sum(jnp.where(order[None, :] < order[:, None], padded[None, :], 0), axis=1)
    blocks = (counts + (ROW_BLOCK - 1)) // ROW_BLOCK
    pair_pos = jnp.sum(jnp.where(hits, place_in.astype(jnp.int32) + starts[None, :], 0), axis=1)
    two = pair_pos.reshape(parts, part_rows, 2)
    rows = pairs + num_experts * (ROW_ALIGN - 1) + ROW_BLOCK
    rows = (rows + GATHER_ROWS - 1) // GATHER_ROWS * GATHER_ROWS
    return starts, blocks, pair_pos, gates.reshape(pairs), two[:, None, :, 0], two[:, None, :, 1], rows


def solution(mesh):
    n_tok, n_mp = mesh.shape['tok'], mesh.shape['mp']
    token_spec = P(('rep', 'tok', 'mp'))
    row_spec = P(('rep', 'tok', 'mp'), None)
    head_weight = P(None, 'tok', 'mp', None)
    in_specs = (row_spec, token_spec, row_spec, row_spec, head_weight, head_weight, head_weight, P(None, 'mp', None, 'tok'), P(None, None, 'tok', 'mp'), P(None, None, 'tok', 'mp'), P(None, None, 'mp', 'tok'), P(None, None), P(None, None))
    swap_perm = [(m * n_tok + t, t * n_tok + m) for t in range(n_tok) for m in range(n_mp)]
    core_perm = [(t, t ^ 1) for t in range(n_tok)]
    y_perm = [(t, t ^ 2) for t in range(n_tok)]
    x_perm = [(0, 1), (1, 0)]

    def swap_roles(value):
        return lax.ppermute(value, ('mp', 'tok'), swap_perm)

    def device_step(hidden_in, seg_ids, expert_ids, expert_gates, w_query, w_key, w_value, w_out, w_gate, w_up, w_down, gain_attn, gain_mlp):
        num_layers, slice_width, q_local, head_dim = w_query.shape
        kv_local = w_key.shape[2]
        groups = q_local // kv_local
        num_experts = w_gate.shape[1]
        half = num_experts // 2
        part_rows = hidden_in.shape[0]
        my_rep, my_tok, my_mp = lax.axis_index('rep'), lax.axis_index('tok'), lax.axis_index('mp')
        place = jnp.stack([my_rep, my_tok]).astype(jnp.int32)
        hidden_width = slice_width * n_tok
        attn_cols = (q_local + 2 * kv_local) * head_dim

        swapped = swap_roles(hidden_in)
        residual = swapped.astype(jnp.float32)
        attn_packs = []
        for layer in range(num_layers):
            qkv = jnp.concatenate([w_query[layer], w_key[layer], w_value[layer]], axis=1).reshape(slice_width, attn_cols)
            pack = jnp.concatenate([qkv, w_out[layer].reshape(q_local * head_dim, slice_width)], axis=1)
            attn_packs.append(swap_roles(pack))

        expert_weights = (w_gate, w_up, w_down)
        peers = []
        for own in expert_weights:
            peers.append(lax.ppermute(own, 'tok', core_perm))
        layer_sets = []
        for layer in range(num_layers):
            sets = []
            for own, peer in zip(expert_weights, peers):
                mine = lax.dynamic_slice(own, (layer, my_rep * half, 0, 0), (1, half) + own.shape[2:])[0]
                y_half = lax.ppermute(mine, 'tok', y_perm)
                x_half = lax.ppermute(y_half, 'rep', x_perm)
                y_far = lax.ppermute(y_half, 'tok', core_perm)
                x_far = lax.ppermute(x_half, 'tok', core_perm)
                sets.append((own, peer, y_half, x_half, y_far, x_far))
            layer_sets.append(sets)

        seg_all = lax.all_gather(seg_ids, ('tok', 'mp'), axis=0)
        pair_info = jnp.concatenate([expert_ids.astype(jnp.float32), expert_gates], axis=1)
        pair_all = lax.all_gather(pair_info, ('tok', 'mp'), axis=0)
        pair_all = pair_all.reshape(n_tok, n_mp, part_rows, 4)
        seg_full = lax.dynamic_index_in_dim(seg_all.reshape(n_tok, n_mp * part_rows), my_mp, axis=0, keepdims=False)
        pair_mine = lax.dynamic_index_in_dim(pair_all, my_tok, axis=1, keepdims=False).reshape(n_tok * part_rows, 4)
        pair_home = lax.dynamic_index_in_dim(pair_all, my_tok, axis=0, keepdims=False).reshape(n_mp * part_rows, 4)
        routes = [routing(info[:, :2].astype(jnp.int32).reshape(-1), info[:, 2:], num_experts, my_rep, n_tok, part_rows) for info in (pair_mine, pair_home)]
        seq_len = seg_full.shape[0]
        token_index = jnp.arange(seq_len, dtype=jnp.int32)
        cosines, sines = rope_tables(request_positions(seg_full), head_dim)
        for layer in range(num_layers):
            pack = lax.all_gather(attn_packs[layer], 'mp', axis=0)
            qkv_weight = pack[:, :, :attn_cols].reshape(hidden_width, attn_cols)
            o_weight = pack[:, :, attn_cols:]
            normed = rms_norm(residual, gain_attn[layer])
            normed = lax.all_gather(normed, 'tok', axis=0, tiled=True)
            qkv = jnp.dot(normed, qkv_weight, preferred_element_type=jnp.float32)
            qkv = qkv.reshape(seq_len, q_local + 2 * kv_local, head_dim)
            rotated = apply_rope(qkv[:, :q_local + kv_local], cosines, sines).astype(jnp.bfloat16)
            q_rot = rotated[:, :q_local].reshape(seq_len, kv_local, groups, head_dim)
            k_rot = rotated[:, q_local:]
            v_all = qkv[:, q_local + kv_local:].astype(jnp.bfloat16)
            attn_out = block_attention(q_rot, k_rot, v_all, seg_full, token_index, seg_full, token_index)
            attn_part = jnp.einsum('sk,tkw->stw', attn_out.reshape(seq_len, q_local * head_dim), o_weight, preferred_element_type=jnp.float32)
            attn_part = attn_part.reshape(seq_len, hidden_width)
            residual = residual + lax.psum_scatter(attn_part, 'tok', scatter_dimension=0, tiled=True)
            normed = rms_norm(residual, gain_mlp[layer])
            last = layer == num_layers - 1
            if last:
                normed = swap_roles(normed)
                residual = swap_roles(residual)
            normed = normed.reshape(part_rows, n_tok, slice_width).transpose(1, 0, 2)
            h_all = lax.all_gather(normed, 'mp', axis=0)
            mix_part = expert_mix(layer, place, routes[int(last)], h_all, layer_sets[layer])
            mix = lax.psum_scatter(mix_part, 'mp', scatter_dimension=0, tiled=True)
            residual = residual + mix.transpose(1, 0, 2).reshape(part_rows, hidden_width)
        return residual

    return jax.shard_map(device_step, mesh=mesh, in_specs=in_specs, out_specs=row_spec, check_vma=False)
```
